32 devices in a mesh: row: 4 (over z), col: 8 (over y, x, core).
Axes of the slice: x: 2, y: 2, z: 4, core: 2. Of those that a mesh axis runs over, the one named last changes fastest.
Arguments:
- matrix: float32 [32, 512, 16, 1024], P(None, 'row', None, 'col'), may hold values from -150 to 150
- inverse_rest: float32 [32, 512, 14, 1024], P(None, 'row', None, 'col'), may hold values from -6 to 6
- upper_block: float32 [4, 512, 2, 1024], P(None, 'row', None, 'col'), may hold values from -6 to 6, as said below
- lower_below: float32 [4, 512, 14, 1024], P(None, 'row', None, 'col'), may hold values from -0.046875 to 0.046875
- lower_inverse: float32 [4, 512, 2048], P(None, 'row', 'col'), may hold values from -1 to 1, as said below
Outputs:
- plus_rows: float32 [4, 512, 16, 1024], P(None, 'row', None, 'col')
The draws below stay inside these ranges and needn't reach their ends.
Inputs may be any that keep to these rules, and one draw needn't show every extreme that they name: `upper_block`: upper triangular. `lower_inverse`: unit lower triangular.
All inputs are finite; a program needn't handle non-finite values.
Results may differ from the reference program's by a relative error of at most 0.000052.
Values sent between devices are 32-bit elements; how exact they have to be, the bound alone decides.
A program may use at most 256 MiB of HBM per device.

```python
import jax
import jax.numpy as jnp
from jax import lax

N = 16384
BLK = 128
W = 2048
REST = 14336
KR = 32
KC = 16
KWR = 4
KW = 2
KCR = 14
N_ROW = 4
N_COL = 8


def draw_matrix(key, part):
    row_key, col_key, base_key = jax.random.split(jax.random.fold_in(key, 17), 3)
    row_scale = jnp.exp(jax.random.uniform(row_key, (N, 1), jnp.float32, 0.0, 2.302585))
    col_scale = jnp.exp(jax.random.uniform(col_key, (1, N), jnp.float32, 0.0, 2.302585))
    values = jnp.clip(jax.random.normal(base_key, (N, N), jnp.float32), -6.0, 6.0)
    return (values * row_scale * col_scale * 0.25).reshape(KR, N // KR, KC, N // KC)


def draw_upper_block(key, part):
    base_key = jax.random.fold_in(key, 23)
    values = jnp.clip(jax.random.normal(base_key, (W, W), jnp.float32), -6.0, 6.0)
    return jnp.triu(values).reshape(KWR, W // KWR, KW, W // KW)


def draw_lower_inverse(key, part):
    base_key = jax.random.fold_in(key, 29)
    values = jnp.clip(jax.random.normal(base_key, (W, W), jnp.float32), -6.0, 6.0) * (0.5 / jnp.sqrt(W * 1.0))
    unit_lower = jnp.eye(W, dtype=jnp.float32) + jnp.tril(values, -1)
    return unit_lower.reshape(KWR, W // KWR, W)


def block_levels(own_key, extent, cuts, smallest, largest):
    loudness = 1.0
    for axis_at, blocks in cuts:
        draws = jax.random.uniform(jax.random.fold_in(jax.random.fold_in(own_key, 6), axis_at), (blocks,), jnp.float32, smallest / len(cuts), largest / len(cuts))
        loudness = loudness * jnp.repeat(jnp.exp(draws), extent[axis_at] // blocks).reshape((-1,) + (1,) * (len(extent) - 1 - axis_at))
    return loudness


def noise(key, dims, spread, reach, pieces=(), held_as=jnp.bfloat16):
    values = spread * jax.random.normal(key, dims, jnp.float32)
    if pieces:
        values = values * block_levels(key, dims, pieces, -0.22, 0.18)
    return jnp.clip(values, -reach, reach).astype(held_as)


def setup_inputs(seed: int = 0) -> dict:
    seeds = jax.random.split(jax.random.key(seed), 6)
    matrix = draw_matrix(jax.random.fold_in(seeds[5], 71), 0)
    inverse_rest = noise(seeds[1], (KR, N_ROW * BLK, KCR, N_COL * BLK), 1.0, 6.0, ((1, 4), (3, 8)), jnp.float32)
    upper_block = draw_upper_block(jax.random.fold_in(seeds[5], 71), 0)
    lower_below = noise(seeds[3], (KWR, N_ROW * BLK, KCR, N_COL * BLK), REST ** -0.5, 0.046875, ((1, 4), (3, 8)), jnp.float32)
    lower_inverse = draw_lower_inverse(jax.random.fold_in(seeds[5], 71), 0)
    return {"matrix": matrix, "inverse_rest": inverse_rest, "upper_block": upper_block, "lower_below": lower_below, "lower_inverse": lower_inverse}


def reference(matrix, inverse_rest, upper_block, lower_below, lower_inverse):
    whole_matrix = matrix.reshape(N, N)
    rest_inverse = inverse_rest.reshape(N, N - W)
    upper_part = upper_block.reshape(W, W)
    below_part = lower_below.reshape(W, N - W)
    factor_part = lower_inverse.reshape(W, W)
    correction = jnp.dot(rest_inverse, below_part.T, precision=lax.Precision.HIGHEST, preferred_element_type=jnp.float32)
    update_panel = jnp.concatenate([upper_part, jnp.zeros((N - W, W), jnp.float32)], axis=0) - correction
    inverse_panel = jnp.dot(update_panel, factor_part, precision=lax.Precision.HIGHEST, preferred_element_type=jnp.float32)
    matrix_norm = jnp.sum(whole_matrix * whole_matrix)
    inverse_norm = jnp.sum(rest_inverse * rest_inverse) + jnp.sum(inverse_panel * inverse_panel)
    balance = jnp.sqrt(jnp.sqrt(inverse_norm / matrix_norm))
    plus_rows = 0.5 * (balance * whole_matrix[:W] + inverse_panel.T / balance)
    return plus_rows.reshape(KWR, W // KWR, KC, N // KC)
```

```python
import jax
import jax.numpy as jnp
from jax import lax
from jax.sharding import PartitionSpec as P


def dot_split(left, right, form):
    return jnp.einsum(
        form, left, right, precision=lax.Precision.HIGH, preferred_element_type=jnp.float32
    )


def mirror(panel_rows, row_devices, col_devices, panel_cycles, blk_size):
    share_rows, col_ratio, width_all = panel_rows.shape
    sectioned = panel_rows.reshape(share_rows, col_ratio, 1, panel_cycles, row_devices, blk_size)
    sectioned = lax.all_to_all(sectioned, "row", split_axis=4, concat_axis=2, tiled=True)
    sectioned = sectioned.reshape(share_rows, col_devices, panel_cycles, blk_size)
    sectioned = lax.all_to_all(sectioned, "col", split_axis=1, concat_axis=0, tiled=True)
    return sectioned.reshape(col_devices * share_rows, panel_cycles * blk_size)


def per_device(matrix, inverse_rest, upper_block, lower_below, lower_inverse):
    row_devices = lax.axis_size("row")
    col_devices = lax.axis_size("col")
    row_at = lax.axis_index("row")
    col_at = lax.axis_index("col")
    col_ratio = col_devices // row_devices
    row_cycles, blk_size, col_cycles, _ = matrix.shape
    panel_cycles = lower_inverse.shape[0]
    width_all = lower_inverse.shape[2] * col_devices
    rest_local = inverse_rest.shape[2] * blk_size
    panel_col_cycles = upper_block.shape[2]
    local_rows = col_cycles * blk_size
    share_rows = local_rows // col_devices
    width_local = panel_cycles * blk_size

    own_below = lower_below.reshape(width_local, rest_local)
    below = [own_below]
    for step in range(1, row_devices):
        pairs = [((at + step) % row_devices, at) for at in range(row_devices)]
        below.append(lax.ppermute(own_below, "row", pairs))

    inverse_rows = inverse_rest.reshape(row_cycles * blk_size, rest_local)
    factor_rows = lax.all_gather(lower_inverse, "row", axis=1, tiled=True)
    factor_all = lax.all_gather(factor_rows, "col", axis=2, tiled=True)
    factor_all = factor_all.reshape(panel_cycles, row_devices, blk_size, width_all)

    upper_rows = upper_block.reshape(width_local, panel_col_cycles, 1, blk_size)
    slot = lax.broadcasted_iota(jnp.int32, (1, 1, col_ratio, 1), 2)
    whole_blocks = share_rows % blk_size == 0

    def scatter_rows(rows):
        if not whole_blocks:
            rows = (
                rows.reshape(col_cycles, col_ratio, blk_size, width_local)
                .transpose(0, 2, 1, 3)
                .reshape(row_cycles * blk_size, width_local)
            )
        return lax.psum_scatter(rows, "col", scatter_dimension=0, tiled=True)

    shares = []
    part = None
    for step in range(row_devices):
        at = lax.rem(row_at + step, row_devices)
        block = below[step]
        if step == 1:
            block, _ = lax.optimization_barrier((block, part))
        if step > 1:
            block, _, _ = lax.optimization_barrier((block, part, shares[step - 2]))
        if step > 0:
            shares.append(scatter_rows(part))
        part = -dot_split(inverse_rows, block, "im,tm->it")
        here = (slot == col_at // row_devices) & (lax.rem(col_at, row_devices) == at)
        spread = jnp.where(here, upper_rows, 0.0).reshape(width_local, width_local)
        part = part.at[:width_local].add(spread)
    shares.append(scatter_rows(part))
    doubled = jnp.concatenate([factor_all, factor_all], axis=1)
    factor = lax.dynamic_slice_in_dim(doubled, row_at, row_devices, axis=1)
    factor = factor.transpose(1, 0, 2, 3).reshape(width_all, width_all)
    total = dot_split(jnp.concatenate(shares, axis=1), factor, "it,tw->iw")
    if whole_blocks:
        inverse_share = (
            total.reshape(share_rows // blk_size, col_ratio, blk_size, width_all)
            .transpose(0, 2, 1, 3)
            .reshape(share_rows, col_ratio, width_all)
        )
    else:
        inverse_share = total.reshape(share_rows, col_ratio, width_all)
    matrix_sq = jnp.sum(matrix * matrix)
    rest_sq = jnp.sum(inverse_rest * inverse_rest)
    panel_sq = jnp.sum(total * total)
    mirrored = mirror(inverse_share, row_devices, col_devices, panel_cycles, blk_size)
    inverse_block = mirrored.reshape(col_cycles, blk_size, panel_cycles, blk_size).transpose(
        2, 3, 0, 1
    )
    matrix_total, inverse_total = lax.psum((matrix_sq, rest_sq + panel_sq), ("row", "col"))
    balance = jnp.sqrt(jnp.sqrt(inverse_total / matrix_total))
    return 0.5 * (balance * matrix[:panel_cycles] + inverse_block / balance)


def solution(mesh):
    in_specs = (
        P(None, "row", None, "col"),
        P(None, "row", None, "col"),
        P(None, "row", None, "col"),
        P(None, "row", None, "col"),
        P(None, "row", "col"),
    )
    out_specs = P(None, "row", None, "col")
    return jax.shard_map(
        per_device, mesh=mesh, in_specs=in_specs, out_specs=out_specs, check_vma=False
    )
```
